512 devices in a mesh: leaf: 16 (over z_lo, core), grp: 8 (over y, z_hi), mrg: 4 (over x).
Axes of the slice: x: 4, y: 4, z: 16 (z_hi: 2, z_lo: 8; z = z_hi * 8 + z_lo), core: 2. Of those that a mesh axis runs over, the one named last changes fastest.
Arguments:
- row_owner: int32 [768], replicated, may hold values from 0 to 767, as said below
- face_left: float32 [8, 4, 768, 768], P('grp', 'mrg', 'leaf'), as said below
- face_cross: float32 [8, 4, 768, 768], P('grp', 'mrg', 'leaf')
- face_right: float32 [8, 4, 768, 768], P('grp', 'mrg', 'leaf')
Outputs:
- out_left: float32 [8, 4, 768, 768], P('grp', 'mrg', 'leaf')
- out_cross: float32 [8, 4, 768, 768], P('grp', 'mrg', 'leaf')
- out_right: float32 [8, 4, 768, 768], P('grp', 'mrg', 'leaf')
The draws below stay inside these ranges and needn't reach their ends.
Inputs may be any that keep to these rules, and one draw needn't show every extreme that they name: row_owner holds each of the 768 face DOFs exactly once. `face_left`: for every box, the symmetric matrix [[L, C], [C^T, R]] built from natural rows is positive definite, L and R are symmetric.
All inputs are finite; a program needn't handle non-finite values.
Results may differ from the reference program's by a relative error of at most 0.0003.
Values sent between devices are 32-bit elements; how exact they have to be, the bound alone decides.
No kernel may reach another device: no remote copies, remote signals or barrier semaphores. Data moves between devices by JAX's collectives and lax.ppermute only.
A program may use at most 128 MiB of HBM per device.

```python
import math
import jax
import jax.numpy as jnp
from jax import lax

F = 768
N_GRP = 8
N_MRG = 4


def shared_order(key):
    return jax.random.permutation(jax.random.fold_in(key, 11), F).astype(jnp.int32)


def half_rows(key, index):
    shape = (N_GRP, N_MRG, F, F)
    sub = jax.random.fold_in(key, 30 + index)
    values = jax.random.normal(sub, shape, jnp.float32)
    return values


def shift_amount(key):
    logs = jax.random.uniform(jax.random.fold_in(key, 40), (N_GRP, N_MRG), jnp.float32, math.log(0.003), math.log(0.01))
    return jnp.exp(logs)


def box_factor(key):
    logs = jax.random.uniform(jax.random.fold_in(key, 50), (N_GRP, N_MRG), jnp.float32, -0.75, 0.75)
    return jnp.exp(logs * math.log(10.0))


def dof_scale(key):
    logs = jax.random.uniform(jax.random.fold_in(key, 60), (F,), jnp.float32, math.log(0.3), 0.0)
    return jnp.exp(logs)


def gram(first, second):
    product = jnp.einsum('gmik,gmjk->gmij', first, second, precision=lax.Precision.HIGHEST)
    return product / (1.0 * F)


def finish(key, block):
    scale = dof_scale(key)
    factor = box_factor(key)
    block = block * scale[None, None, :, None] * scale[None, None, None, :]
    block = block * factor[:, :, None, None]
    return jnp.take(block, shared_order(key), axis=2)


def draw_row_owner(key, part):
    return shared_order(key)


def draw_face_left(key, part):
    upper = half_rows(key, 1)
    block = gram(upper, upper) + shift_amount(key)[:, :, None, None] * jnp.eye(F, dtype=jnp.float32)
    return finish(key, block)


def draw_face_right(key, part):
    lower = half_rows(key, 2)
    block = gram(lower, lower) + shift_amount(key)[:, :, None, None] * jnp.eye(F, dtype=jnp.float32)
    return finish(key, block)


def draw_face_cross(key, part):
    block = gram(half_rows(key, 1), half_rows(key, 2))
    return finish(key, block)


def setup_inputs(seed: int = 0) -> dict:
    seeds = jax.random.split(jax.random.key(seed), 5)
    return {
        "row_owner": draw_row_owner(jax.random.fold_in(seeds[4], 71), 0),
        "face_left": draw_face_left(jax.random.fold_in(seeds[4], 71), 0),
        "face_cross": draw_face_cross(jax.random.fold_in(seeds[4], 71), 0),
        "face_right": draw_face_right(jax.random.fold_in(seeds[4], 71), 0),
    }


def dot_high(left, right):
    return jnp.dot(left.astype(jnp.float32), right.astype(jnp.float32), precision=lax.Precision.HIGHEST, preferred_element_type=jnp.float32)

def merge(first, second):
    interface = first[2] + second[0]
    factor = jnp.linalg.cholesky(interface)
    solved = jax.scipy.linalg.cho_solve((factor, True), first[1].T).T
    weights = jax.scipy.linalg.cho_solve((factor, True), second[1])
    new_left = first[0] - dot_high(solved, first[1].T)
    new_cross = -dot_high(solved, second[1])
    new_right = second[2] - dot_high(second[1].T, weights)
    return jnp.stack([new_left, new_cross, new_right])

def reference(row_owner, face_left, face_cross, face_right):
    width = face_left.shape[2]
    inverse_map = jnp.zeros((width,), jnp.int32).at[row_owner].set(jnp.arange(width, dtype=jnp.int32))
    boxes = jnp.stack([face_left, face_cross, face_right], axis=2)
    boxes = jnp.take(boxes, inverse_map, axis=3)
    level_one = jax.vmap(jax.vmap(merge))(boxes[0::2], boxes[1::2])
    level_two = jax.vmap(jax.vmap(merge))(level_one[:, 0::2], level_one[:, 1::2])
    whole = jnp.repeat(jnp.repeat(level_two, 2, axis=0), 2, axis=1)
    whole = jnp.take(whole, row_owner, axis=3)
    return (whole[:, :, 0], whole[:, :, 1], whole[:, :, 2])
```

```python
import functools

import jax
import jax.numpy as jnp
from jax import lax
from jax.experimental import pallas as pl
from jax.experimental.pallas import tpu as pltpu
from jax.sharding import Mesh
from jax.sharding import PartitionSpec as P

F = 768
ROWS = 48
HALF = 384
B = 128
F32 = jnp.float32
BF16 = jnp.bfloat16
PAIR = ("zh", "zl", "core")
SWAP = [(0, 1), (1, 0)]
VMEM = pl.BlockSpec(memory_space=pltpu.VMEM)
ANY = pl.BlockSpec(memory_space=pl.ANY)


def params(mib):
    return pltpu.CompilerParams(vmem_limit_bytes=mib * 1024 * 1024)


def dg(a, b, dims):
    return lax.dot_general(a, b, (dims, ((), ())), preferred_element_type=F32)


NN = ((1,), (0,))
NT = ((1,), (1,))
TN = ((0,), (0,))
TT = ((0,), (1,))


def split2(x):
    h = x.astype(BF16)
    return h, (x - h.astype(F32)).astype(BF16)


def split3(x):
    h = x.astype(BF16)
    y = x - h.astype(F32)
    m = y.astype(BF16)
    return h, m, (y - m.astype(F32)).astype(BF16)


def mul3(a, b, dims):
    return (dg(a[1], b[0], dims) + dg(a[0], b[1], dims)) + dg(a[0], b[0], dims)


def pick(x, onehot, dims):
    h, m, l = split3(x)
    return (dg(l, onehot, dims) + dg(m, onehot, dims)) + dg(h, onehot, dims)


def onehot_of(ro):
    c = lax.broadcasted_iota(jnp.int32, (F, F), 0)
    return jnp.where(c == ro, 1.0, 0.0).astype(BF16)


def sub(v, s):
    return jnp.broadcast_to(v[s : s + 1, :], v.shape)


def lane(v, j):
    return jnp.broadcast_to(v[:, j : j + 1], v.shape)


def inv8(b, row):
    b = list(b)
    for p in range(4):
        i, k = 2 * p, 2 * p + 1
        a_, b_, d_ = sub(b[i], i), sub(b[k], i), sub(b[k], k)
        rd = 1.0 / (a_ * d_ - b_ * b_)
        pa, pb, pd = d_ * rd, -b_ * rd, a_ * rd
        ci = jnp.where(row == i, -1.0, jnp.where(row == k, 0.0, b[i]))
        ck = jnp.where(row == k, -1.0, jnp.where(row == i, 0.0, b[k]))
        ui = ci * pa + ck * pb
        uk = ci * pb + ck * pd
        keep = (row != i) & (row != k)
        new = []
        for j in range(8):
            if j == i:
                new.append(-ui)
            elif j == k:
                new.append(-uk)
            else:
                base = jnp.where(keep, b[j], 0.0)
                new.append(base - (ui * sub(b[j], i) + uk * sub(b[j], k)))
        b = new
    return b


def tree(u):
    return ((u[0] + u[1]) + (u[2] + u[3])) + ((u[4] + u[5]) + (u[6] + u[7]))


def inv128(D):
    row = lax.broadcasted_iota(jnp.int32, (8, B), 0)
    col = lax.broadcasted_iota(jnp.int32, (8, B), 1)
    D = list(D)
    for r in range(16):
        rows = D[r]
        ib = inv8([lane(rows, 8 * r + j) for j in range(8)], row)
        inp = (col >= 8 * r) & (col < 8 * r + 8)
        rows = jnp.where(inp, jnp.where(col - 8 * r == row, 1.0, 0.0), rows)
        T = tree([ib[j] * sub(rows, j) for j in range(8)])
        Tj = [sub(T, j) for j in range(8)]
        for q in list(range(r + 1, 16)) + list(range(r)):
            u = tree([lane(D[q], 8 * r + j) * Tj[j] for j in range(8)])
            D[q] = jnp.where(inp, 0.0, D[q]) - u
        D[r] = T
    return D


def cat(*a, axis):
    return jnp.concatenate(a, axis=axis)


def mul6(a, b):
    a0, a1, a2 = split3(a)
    b0, b1, b2 = split3(b)
    a01 = cat(a0, a1, axis=1)
    low = dg(cat(a0, a2, axis=1), cat(b2, b0, axis=0), NN) + dg(a01, cat(b1, b1, axis=0), NN)
    return low + dg(a01, cat(b0, b0, axis=0), NN)


def invert(s_ref, d_ref, di_ref, r_ref, c_ref):
    ri = lax.broadcasted_iota(jnp.int32, (B, B), 0)
    ci = lax.broadcasted_iota(jnp.int32, (B, B), 1)
    eye = jnp.where(ri == ci, 1.0, 0.0)
    last = F // B - 1
    di_ref[...] = jnp.zeros((B, B), F32)
    r_ref[...] = jnp.zeros((B, F), F32)
    c_ref[...] = jnp.zeros((F, B), F32)
    d_ref[...] = s_ref[:B, :B]

    def trail(kp):
        T = mul6(di_ref[...], r_ref[...])
        t0, t1 = split2(T)
        c0, c1 = split2(c_ref[...])
        lhs = cat(c0, c1, axis=1)
        rhs = cat(t0, t0, axis=0)
        for j in range(F // 256):
            js = slice(256 * j, 256 * j + 256)
            s_ref[:F, js] = s_ref[:F, js] - (dg(lhs, rhs[:, js], NN) + dg(c0, t1[:, js], NN))
        s_ref[pl.ds(kp, B), :] = T

    def step(k, carry):
        ks = pl.multiple_of(k * B, B)
        kp = pl.multiple_of(jnp.where(k == 0, F, ks - B), B)
        kn = pl.multiple_of(jnp.where(k == last, F - B, ks + B), B)
        Di = jnp.concatenate(inv128([d_ref[8 * q : 8 * q + 8, :] for q in range(16)]), axis=0)
        trail(kp)
        rn = s_ref[pl.ds(ks, B), pl.ds(kn, B)]
        cn = s_ref[pl.ds(kn, B), pl.ds(ks, B)]
        dn = s_ref[pl.ds(kn, B), pl.ds(kn, B)]
        c_ref[...] = s_ref[:F, pl.ds(ks, B)]
        c_ref[pl.ds(ks, B), :] = jnp.zeros((B, B), F32)
        r_ref[...] = s_ref[pl.ds(ks, B), :]
        r_ref[:, pl.ds(ks, B)] = eye
        s_ref[:F, pl.ds(ks, B)] = jnp.zeros((F, B), F32)
        di_ref[...] = Di
        t0, t1 = split2(mul6(Di, rn))
        c0, c1 = split2(cn)
        d_ref[...] = dn - (dg(cat(c0, c1, axis=1), cat(t0, t0, axis=0), NN) + dg(c0, t1, NN))
        return carry

    lax.fori_loop(0, last + 1, step, 0)
    trail(F - B)


INVERT_SCRATCH = [
    pltpu.VMEM((F + B, F), F32),
    pltpu.VMEM((B, B), F32),
    pltpu.VMEM((B, B), F32),
    pltpu.VMEM((B, F), F32),
    pltpu.VMEM((F, B), F32),
]


def enter_body(ro, left, cross, right, send, other):
    p = onehot_of(ro[...])
    upper = lax.axis_index("zh") == 1
    l, c, r = left[...], cross[...], right[...]
    send[0] = pick(jnp.where(upper, l, r), p, NN)
    send[1] = pick(c, p, NN)
    other[...] = pick(jnp.where(upper, r, l), p, NN)


def enter(ro, left, cross, right):
    return pl.pallas_call(
        enter_body,
        out_shape=(jax.ShapeDtypeStruct((2, ROWS, F), F32), jax.ShapeDtypeStruct((ROWS, F), F32)),
        in_specs=[VMEM] * 4,
        out_specs=(VMEM, VMEM),
        compiler_params=params(32),
        name="enter",
    )(ro, left, cross, right)


def level_one_body(g, v_out, t_out, si_out, a_ref, c_ref, t_ref, sems, s_ref, *work):
    ga = pltpu.make_async_copy(g.at[0], a_ref, sems.at[0])
    gc = pltpu.make_async_copy(g.at[1], c_ref, sems.at[1])
    ga.start()
    gc.start()
    ga.wait()
    s_ref[:F, :] = a_ref[:F, :] + a_ref[F:, :]
    invert(s_ref, *work)
    gc.wait()
    si_out[...] = s_ref[:F, :]
    si = split2(s_ref[:F, :])
    h = pl.multiple_of(lax.axis_index("core") * HALF, HALF)
    low = lax.axis_index("xl") == 0

    @pl.when(low)
    def _():
        cb = split2(c_ref[F:, :])
        t = mul3(si, cb, NN)
        t_out[...] = t
        part = split2(c_ref[F:, pl.ds(h, HALF)])
        v_out[...] = mul3(part, split2(t), TN)

    @pl.when(jnp.logical_not(low))
    def _():
        ca = split2(c_ref[:F, :])
        t_ref[...] = mul3(ca, si, NN)
        t_out[...] = t_ref[...]
        part = split2(t_ref[pl.ds(h, HALF), :])
        v_out[...] = mul3(part, ca, NT)


def level_one(g):
    mat = jax.ShapeDtypeStruct((F, F), F32)
    return pl.pallas_call(
        level_one_body,
        out_shape=(jax.ShapeDtypeStruct((HALF, F), F32), mat, mat),
        in_specs=[ANY],
        out_specs=(VMEM, VMEM, VMEM),
        scratch_shapes=[
            pltpu.VMEM((2 * F, F), F32),
            pltpu.VMEM((2 * F, F), F32),
            pltpu.VMEM((F, F), F32),
            pltpu.SemaphoreType.DMA((2,)),
        ]
        + INVERT_SCRATCH,
        compiler_params=params(56),
        cost_estimate=pl.CostEstimate(flops=40 * 10**9, transcendentals=0, bytes_accessed=12 * 10**6),
        name="level_one",
    )(g)


def between_body(g, t, si, keep, m_out, base_out, a_out, c_ref, sems):
    gc = pltpu.make_async_copy(g.at[1], c_ref, sems.at[0])
    gc.start()
    gc.wait()
    i = (lax.axis_index("zl") * 2 + lax.axis_index("core")) * ROWS
    i = pl.multiple_of(i, ROWS)
    low = lax.axis_index("xl") == 0
    tt = split2(t[...])
    sis = split2(si[...])
    ca = split2(c_ref[:F, :])
    cb = split2(c_ref[F:, :])

    @pl.when(low)
    def _():
        rows = split2(c_ref[pl.ds(i, ROWS), :])
        y = mul3(rows, sis, NN)
        base_out[...] = keep[...] - mul3(split2(y), ca, NT)
        a_out[...] = -mul3(rows, tt, NN)
        m_out[...] = -mul3(tt, ca, TT)

    @pl.when(jnp.logical_not(low))
    def _():
        r_ = lax.broadcasted_iota(jnp.int32, (ROWS, F), 0) + i
        c_ = lax.broadcasted_iota(jnp.int32, (ROWS, F), 1)
        e = jnp.where(r_ == c_, 1.0, 0.0).astype(BF16)
        rows = (dg(e, cb[0], NT).astype(BF16), dg(e, cb[1], NT).astype(BF16))
        y = mul3(rows, sis, NN)
        base_out[...] = keep[...] - mul3(split2(y), cb, NN)
        a_out[...] = -mul3(rows, tt, NT)
        m_out[...] = -mul3(tt, cb, NN)


def between(g, t, si, keep):
    rows = jax.ShapeDtypeStruct((ROWS, F), F32)
    return pl.pallas_call(
        between_body,
        out_shape=(jax.ShapeDtypeStruct((F, F), F32), rows, rows),
        in_specs=[ANY, VMEM, VMEM, VMEM],
        out_specs=(VMEM, VMEM, VMEM),
        scratch_shapes=[pltpu.VMEM((2 * F, F), F32), pltpu.SemaphoreType.DMA((1,))],
        compiler_params=params(56),
        cost_estimate=pl.CostEstimate(flops=6 * 10**9, transcendentals=0, bytes_accessed=12 * 10**6),
        name="between",
    )(g, t, si, keep)


def level_two_body(q, mine, theirs, m, base, a, b, ro, out, m_ref, q_ref, sems, s_ref, *work):
    gq = pltpu.make_async_copy(q, q_ref, sems.at[0])
    gm = pltpu.make_async_copy(m, m_ref, sems.at[1])
    gq.start()
    gm.start()
    gq.wait()
    core = lax.axis_index("core")
    for k in range(16):
        for z in range(2):
            s_ref[48 * k + 24 * z : 48 * k + 24 * z + 24, :] = q_ref[z, k]
    h = pl.multiple_of(core * HALF, HALF)
    o = pl.multiple_of((1 - core) * HALF, HALF)
    s_ref[pl.ds(h, HALF), :] = s_ref[pl.ds(h, HALF), :] - mine[...]
    s_ref[pl.ds(o, HALF), :] = s_ref[pl.ds(o, HALF), :] - theirs[...]
    invert(s_ref, *work)
    gm.wait()
    low = lax.axis_index("xl") == 0
    x = jnp.concatenate([jnp.where(low, a[...], b[...]), a[...]], axis=0)
    y = mul3(split2(x), split2(s_ref[:F, :]), NN)
    z = mul3(split2(y), split2(m_ref[...]), NN)
    first = jnp.where(low, base[...], 0.0) - z[:ROWS]
    second = base[...] - z[ROWS:]
    p = onehot_of(ro[...])
    out[...] = pick(jnp.concatenate([first, second], axis=0), p, NT)


def level_two(q, mine, theirs, m, base, a, b, ro):
    return pl.pallas_call(
        level_two_body,
        out_shape=jax.ShapeDtypeStruct((2 * ROWS, F), F32),
        in_specs=[ANY, VMEM, VMEM, ANY, VMEM, VMEM, VMEM, VMEM],
        out_specs=VMEM,
        scratch_shapes=[
            pltpu.VMEM((F, F), F32),
            pltpu.VMEM((2, 16, 24, F), F32),
            pltpu.SemaphoreType.DMA((2,)),
        ]
        + INVERT_SCRATCH,
        compiler_params=params(56),
        cost_estimate=pl.CostEstimate(flops=40 * 10**9, transcendentals=0, bytes_accessed=12 * 10**6),
        name="level_two",
    )(q, mine, theirs, m, base, a, b, ro)


def shards(row_owner, face_left, face_cross, face_right):
    ro = row_owner.reshape(1, F)
    zh = lax.axis_index("zh")
    xl = lax.axis_index("xl")
    send, other = enter(ro, face_left[0, 0], face_cross[0, 0], face_right[0, 0])
    g = lax.all_gather(send, PAIR, axis=1, tiled=True)
    partner = lax.ppermute(other, "zh", SWAP)
    own = zh == xl
    keep = jnp.where(own, other, partner)
    give = jnp.where(own, partner, other)
    q = give + lax.ppermute(give, "xl", SWAP)
    q = lax.dynamic_slice_in_dim(q, zh * 24, 24, 0)
    q = lax.all_gather(q, PAIR, axis=0, tiled=True).reshape(2, 16, 24, F)
    v, t, si = level_one(g)
    v2 = lax.ppermute(v, "xl", SWAP)
    m, base, a = between(g, t, si, keep)
    b = lax.ppermute(a, "xl", SWAP)
    v2, m, base, a, b = lax.optimization_barrier((v2, m, base, a, b))
    w = v + v2
    w2 = lax.ppermute(w, "core", SWAP)
    mine = level_two(q, w, w2, m, base, a, b, ro)
    theirs = lax.ppermute(mine, "xl", SWAP)
    low = xl == 0
    left = jnp.where(low, mine[:ROWS], theirs[:ROWS])
    cross = jnp.where(low, theirs[:ROWS], mine[:ROWS])
    right = jnp.where(low, theirs[ROWS:], mine[ROWS:])
    return (left[None, None], cross[None, None], right[None, None])


def solution(mesh):
    fine = Mesh(mesh.devices.reshape(8, 2, 4, 2, 2, 2), ("zl", "core", "y", "zh", "xh", "xl"))
    face = P(("y", "zh"), ("xh", "xl"), ("zl", "core"), None)
    return jax.shard_map(
        shards, mesh=fine, in_specs=(P(), face, face, face), out_specs=(face, face, face), check_vma=False
    )
```

```python
import functools

import jax
import jax.numpy as jnp
from jax import lax
from jax.experimental import pallas as pl
from jax.experimental.pallas import tpu as pltpu
from jax.sharding import Mesh
from jax.sharding import PartitionSpec as P

F = 768
ROWS = 48
B = 128
F32 = jnp.float32
BF16 = jnp.bfloat16
PAIR = ("zh", "zl", "core")
SWAP = [(0, 1), (1, 0)]
VMEM = pl.BlockSpec(memory_space=pltpu.VMEM)
ANY = pl.BlockSpec(memory_space=pl.ANY)


def params(mib):
    return pltpu.CompilerParams(vmem_limit_bytes=mib * 1024 * 1024)


def dg(a, b, dims):
    return lax.dot_general(a, b, (dims, ((), ())), preferred_element_type=F32)


NN = ((1,), (0,))
NT = ((1,), (1,))
TN = ((0,), (0,))
TT = ((0,), (1,))


def split2(x):
    h = x.astype(BF16)
    return h, (x - h.astype(F32)).astype(BF16)


def split3(x):
    h = x.astype(BF16)
    y = x - h.astype(F32)
    m = y.astype(BF16)
    return h, m, (y - m.astype(F32)).astype(BF16)


def mul3(a, b, dims):
    return (dg(a[1], b[0], dims) + dg(a[0], b[1], dims)) + dg(a[0], b[0], dims)


def mul6full(a, b):
    low = (dg(a[2], b[0], NN) + dg(a[0], b[2], NN)) + dg(a[1], b[1], NN)
    return (low + (dg(a[1], b[0], NN) + dg(a[0], b[1], NN))) + dg(a[0], b[0], NN)


def mul_into(out_ref, x_ref, y_ref, xh_ref, xl_ref):
    xh_ref[...], xl_ref[...] = split2(x_ref[...])

    def tile(j, carry):
        js = pl.ds(pl.multiple_of(j * 256, 256), 256)
        out_ref[:, js] = mul3((xh_ref[...], xl_ref[...]), split2(y_ref[:, js]), NN)
        return carry

    lax.fori_loop(0, F // 256, tile, 0)


def pick(x, onehot, dims):
    h, m, l = split3(x)
    return (dg(l, onehot, dims) + dg(m, onehot, dims)) + dg(h, onehot, dims)


def onehot_of(ro):
    c = lax.broadcasted_iota(jnp.int32, (F, F), 0)
    return jnp.where(c == ro, 1.0, 0.0).astype(BF16)


def sub(v, s):
    return jnp.broadcast_to(v[s : s + 1, :], v.shape)


def lane(v, j):
    return jnp.broadcast_to(v[:, j : j + 1], v.shape)


def inv8(b, row):
    b = list(b)
    for p in range(4):
        i, k = 2 * p, 2 * p + 1
        a_, b_, d_ = sub(b[i], i), sub(b[k], i), sub(b[k], k)
        rd = 1.0 / (a_ * d_ - b_ * b_)
        pa, pb, pd = d_ * rd, -b_ * rd, a_ * rd
        ci = jnp.where(row == i, -1.0, jnp.where(row == k, 0.0, b[i]))
        ck = jnp.where(row == k, -1.0, jnp.where(row == i, 0.0, b[k]))
        ui = ci * pa + ck * pb
        uk = ci * pb + ck * pd
        keep = (row != i) & (row != k)
        new = []
        for j in range(8):
            if j == i:
                new.append(-ui)
            elif j == k:
                new.append(-uk)
            else:
                base = jnp.where(keep, b[j], 0.0)
                new.append(base - (ui * sub(b[j], i) + uk * sub(b[j], k)))
        b = new
    return b


def tree(u):
    return ((u[0] + u[1]) + (u[2] + u[3])) + ((u[4] + u[5]) + (u[6] + u[7]))


def inv128(D):
    row = lax.broadcasted_iota(jnp.int32, (8, B), 0)
    col = lax.broadcasted_iota(jnp.int32, (8, B), 1)
    D = list(D)
    for r in range(16):
        rows = D[r]
        ib = inv8([lane(rows, 8 * r + j) for j in range(8)], row)
        inp = (col >= 8 * r) & (col < 8 * r + 8)
        rows = jnp.where(inp, jnp.where(col - 8 * r == row, 1.0, 0.0), rows)
        T = tree([ib[j] * sub(rows, j) for j in range(8)])
        Tj = [sub(T, j) for j in range(8)]
        for q in list(range(r + 1, 16)) + list(range(r)):
            u = tree([lane(D[q], 8 * r + j) * Tj[j] for j in range(8)])
            D[q] = jnp.where(inp, 0.0, D[q]) - u
        D[r] = T
    return D


def cat(*a, axis):
    return jnp.concatenate(a, axis=axis)


def mul6(a, b):
    a0, a1, a2 = split3(a)
    b0, b1, b2 = split3(b)
    a01 = cat(a0, a1, axis=1)
    low = dg(cat(a0, a2, axis=1), cat(b2, b0, axis=0), NN) + dg(a01, cat(b1, b1, axis=0), NN)
    return low + dg(a01, cat(b0, b0, axis=0), NN)


def invert(s_ref, d_ref, di_ref, r_ref, c_ref):
    ri = lax.broadcasted_iota(jnp.int32, (B, B), 0)
    ci = lax.broadcasted_iota(jnp.int32, (B, B), 1)
    eye = jnp.where(ri == ci, 1.0, 0.0)
    last = F // B - 1
    di_ref[...] = jnp.zeros((B, B), F32)
    r_ref[...] = jnp.zeros((B, F), F32)
    c_ref[...] = jnp.zeros((F, B), F32)
    d_ref[...] = s_ref[:B, :B]

    def trail(kp):
        T = mul6(di_ref[...], r_ref[...])
        t0, t1 = split2(T)
        c0, c1 = split2(c_ref[...])
        lhs = cat(c0, c1, axis=1)
        rhs = cat(t0, t0, axis=0)
        for j in range(F // 256):
            js = slice(256 * j, 256 * j + 256)
            s_ref[:F, js] = s_ref[:F, js] - (dg(lhs, rhs[:, js], NN) + dg(c0, t1[:, js], NN))
        s_ref[pl.ds(kp, B), :] = T

    def step(k, carry):
        ks = pl.multiple_of(k * B, B)
        kp = pl.multiple_of(jnp.where(k == 0, F, ks - B), B)
        kn = pl.multiple_of(jnp.where(k == last, F - B, ks + B), B)
        Di = jnp.concatenate(inv128([d_ref[8 * q : 8 * q + 8, :] for q in range(16)]), axis=0)
        trail(kp)
        rn = s_ref[pl.ds(ks, B), pl.ds(kn, B)]
        cn = s_ref[pl.ds(kn, B), pl.ds(ks, B)]
        dn = s_ref[pl.ds(kn, B), pl.ds(kn, B)]
        c_ref[...] = s_ref[:F, pl.ds(ks, B)]
        c_ref[pl.ds(ks, B), :] = jnp.zeros((B, B), F32)
        r_ref[...] = s_ref[pl.ds(ks, B), :]
        r_ref[:, pl.ds(ks, B)] = eye
        s_ref[:F, pl.ds(ks, B)] = jnp.zeros((F, B), F32)
        di_ref[...] = Di
        t0, t1 = split2(mul6(Di, rn))
        c0, c1 = split2(cn)
        d_ref[...] = dn - (dg(cat(c0, c1, axis=1), cat(t0, t0, axis=0), NN) + dg(c0, t1, NN))
        return carry

    lax.fori_loop(0, last + 1, step, 0)
    trail(F - B)


INVERT_SCRATCH = [
    pltpu.VMEM((F + B, F), F32),
    pltpu.VMEM((B, B), F32),
    pltpu.VMEM((B, B), F32),
    pltpu.VMEM((B, F), F32),
    pltpu.VMEM((F, B), F32),
]


def enter_body(ro, left, cross, right, send, part):
    p = onehot_of(ro[...])
    upper = lax.axis_index("zh") == 1
    l, c, r = left[...], cross[...], right[...]
    part[...] = pick(jnp.where(upper, l, r), p, NN)
    send[0] = pick(c, p, NN)
    send[1] = pick(jnp.where(upper, r, l), p, NN)


def enter(ro, left, cross, right):
    return pl.pallas_call(
        enter_body,
        out_shape=(jax.ShapeDtypeStruct((2, ROWS, F), F32), jax.ShapeDtypeStruct((ROWS, F), F32)),
        in_specs=[VMEM] * 4,
        out_specs=(VMEM, VMEM),
        compiler_params=params(32),
        name="enter",
    )(ro, left, cross, right)


def level_one_body(mine, theirs, si_out, s_ref, *work):
    core = lax.axis_index("core")
    zl = lax.axis_index("zl")
    for k in range(8):
        at = lax.rem(zl + k, 8) * (2 * ROWS)
        s_ref[pl.ds(pl.multiple_of(at + core * ROWS, ROWS), ROWS), :] = mine[ROWS * k : ROWS * k + ROWS, :]
        s_ref[pl.ds(pl.multiple_of(at + (1 - core) * ROWS, ROWS), ROWS), :] = theirs[ROWS * k : ROWS * k + ROWS, :]
    invert(s_ref, *work)
    si_out[...] = s_ref[:F, :]


def level_one(mine, theirs):
    return pl.pallas_call(
        level_one_body,
        out_shape=jax.ShapeDtypeStruct((F, F), F32),
        in_specs=[VMEM, VMEM],
        out_specs=VMEM,
        scratch_shapes=INVERT_SCRATCH,
        compiler_params=params(40),
        cost_estimate=pl.CostEstimate(flops=40 * 10**9, transcendentals=0, bytes_accessed=5 * 10**6),
        name="level_one",
    )(mine, theirs)


def products_body(si, g, w_out, t_out, x_ref, y_ref, o_ref, t_ref, xh_ref, xl_ref, sems):
    low = lax.axis_index("xl") == 0
    first = lax.axis_index("core") == 0
    go = pltpu.make_async_copy(g.at[1, pl.ds(pl.multiple_of(jnp.where(low, F, 0), F), F)], o_ref, sems.at[2])

    @pl.when(low)
    def _():
        pltpu.make_async_copy(si, x_ref, sems.at[0]).start()
        pltpu.make_async_copy(g.at[0, F:], y_ref, sems.at[1]).start()

    @pl.when(jnp.logical_not(low))
    def _():
        pltpu.make_async_copy(g.at[0, :F], x_ref, sems.at[0]).start()
        pltpu.make_async_copy(si, y_ref, sems.at[1]).start()

    go.start()
    pltpu.make_async_copy(si, x_ref, sems.at[0]).wait()
    pltpu.make_async_copy(si, y_ref, sems.at[1]).wait()
    mul_into(t_ref, x_ref, y_ref, xh_ref, xl_ref)
    out = pltpu.make_async_copy(t_ref, t_out, sems.at[0])
    out.start()
    go.wait()

    def panels(block):
        @pl.when(first)
        def _():
            w_out[:, :768] = o_ref[:B, :] - block(0)
            w_out[:, 768:] = o_ref[B : 2 * B, B:] - block(1)

        @pl.when(jnp.logical_not(first))
        def _():
            w_out[:, :512] = o_ref[2 * B : 3 * B, 2 * B :] - block(2)
            w_out[:, 512:896] = o_ref[3 * B : 4 * B, 3 * B :] - block(3)
            w_out[:, 896:1152] = o_ref[4 * B : 5 * B, 4 * B :] - block(4)
            w_out[:, 1152:1280] = o_ref[5 * B :, 5 * B :] - block(5)
            w_out[:, 1280:] = jnp.zeros((B, B), F32)

    @pl.when(low)
    def _():
        panels(lambda i: mul3(split2(y_ref[:, B * i : B * i + B]), split2(t_ref[:, B * i :]), TN))

    @pl.when(jnp.logical_not(low))
    def _():
        panels(
            lambda i: mul3(split2(t_ref[B * i : B * i + B, :]), (xh_ref[B * i :, :], xl_ref[B * i :, :]), NT)
        )

    out.wait()


def products(si, g):
    return pl.pallas_call(
        products_body,
        out_shape=(jax.ShapeDtypeStruct((B, 11 * B), F32), jax.ShapeDtypeStruct((F, F), F32)),
        in_specs=[ANY, ANY],
        out_specs=(VMEM, ANY),
        scratch_shapes=[pltpu.VMEM((F, F), F32)] * 4
        + [pltpu.VMEM((F, F), BF16)] * 2
        + [pltpu.SemaphoreType.DMA((3,))],
        compiler_params=params(56),
        cost_estimate=pl.CostEstimate(flops=6 * 10**9, transcendentals=0, bytes_accessed=12 * 10**6),
        name="products",
    )(si, g)


def between_body(g, t, si, m_out, base_out, a_out, x_ref, y_ref, s_ref, m_ref, xh_ref, xl_ref, keep, sems):
    low = lax.axis_index("xl") == 0
    i = (lax.axis_index("zl") * 2 + lax.axis_index("core")) * ROWS
    i = pl.multiple_of(i, ROWS)
    gk = pltpu.make_async_copy(
        g.at[1, pl.ds(pl.multiple_of(i + jnp.where(low, 0, F), ROWS), ROWS)], keep, sems.at[2]
    )
    gs = pltpu.make_async_copy(si, s_ref, sems.at[3])

    @pl.when(low)
    def _():
        pltpu.make_async_copy(g.at[0, :F], x_ref, sems.at[0]).start()
        pltpu.make_async_copy(t, y_ref, sems.at[1]).start()

    @pl.when(jnp.logical_not(low))
    def _():
        pltpu.make_async_copy(t, x_ref, sems.at[0]).start()
        pltpu.make_async_copy(g.at[0, F:], y_ref, sems.at[1]).start()

    gk.start()
    gs.start()
    pltpu.make_async_copy(t, x_ref, sems.at[0]).wait()
    pltpu.make_async_copy(t, y_ref, sems.at[1]).wait()
    mul_into(m_ref, x_ref, y_ref, xh_ref, xl_ref)
    out = pltpu.make_async_copy(m_ref, m_out, sems.at[0])
    out.start()
    gk.wait()
    gs.wait()
    s = split2(s_ref[...])

    @pl.when(low)
    def _():
        rows = (xh_ref[pl.ds(i, ROWS), :], xl_ref[pl.ds(i, ROWS), :])
        z = mul3(rows, s, NN)
        base_out[...] = keep[...] - mul3(split2(z), (xh_ref[...], xl_ref[...]), NT)
        a_out[...] = m_ref[pl.ds(i, ROWS), :]

    @pl.when(jnp.logical_not(low))
    def _():
        r_ = lax.broadcasted_iota(jnp.int32, (ROWS, F), 0) + i
        c_ = lax.broadcasted_iota(jnp.int32, (ROWS, F), 1)
        e = jnp.where(r_ == c_, 1.0, 0.0).astype(BF16)
        y = split2(y_ref[...])
        rows = (dg(e, y[0], NT).astype(BF16), dg(e, y[1], NT).astype(BF16))
        z = mul3(rows, s, NN)
        base_out[...] = keep[...] - mul3(split2(z), y, NN)
        h, k, l = split3(m_ref[...])
        a_out[...] = (dg(e, l, NT) + dg(e, k, NT)) + dg(e, h, NT)

    out.wait()


def between(g, t, si):
    rows = jax.ShapeDtypeStruct((ROWS, F), F32)
    return pl.pallas_call(
        between_body,
        out_shape=(jax.ShapeDtypeStruct((F, F), F32), rows, rows),
        in_specs=[ANY, ANY, ANY],
        out_specs=(ANY, VMEM, VMEM),
        scratch_shapes=[pltpu.VMEM((F, F), F32)] * 4
        + [pltpu.VMEM((F, F), BF16)] * 2
        + [pltpu.VMEM((ROWS, F), F32), pltpu.SemaphoreType.DMA((4,))],
        compiler_params=params(56),
        cost_estimate=pl.CostEstimate(flops=6 * 10**9, transcendentals=0, bytes_accessed=12 * 10**6),
        name="between",
    )(g, t, si)


def level_two_body(mine, theirs, m, base, a, b, ro, out, m_ref, z_ref, sems, s_ref, *work):
    gm = pltpu.make_async_copy(m, m_ref, sems.at[0])
    gm.start()
    first = lax.axis_index("core") == 0
    upper = jnp.where(first, mine[...], theirs[...])
    lower = jnp.where(first, theirs[...], mine[...])
    rows = [
        upper[:, :768],
        upper[:, 768:],
        lower[:, :512],
        lower[:, 512:896],
        lower[:, 896:1152],
        lower[:, 1152:1280],
    ]
    for i in range(6):
        s_ref[B * i : B * i + B, B * i :] = rows[i]
        for j in range(i + 1, 6):
            s_ref[B * j : B * j + B, B * i : B * i + B] = rows[i][:, B * (j - i) : B * (j - i) + B].T
    invert(s_ref, *work)
    gm.wait()
    low = lax.axis_index("xl") == 0
    x = jnp.concatenate([jnp.where(low, a[...], b[...]), a[...]], axis=0)
    y = mul6full(split3(x), split3(s_ref[:F, :]))
    ys = split2(y)
    ms = split2(m_ref[...])

    @pl.when(low)
    def _():
        z_ref[...] = mul3(ys, ms, NT)

    @pl.when(jnp.logical_not(low))
    def _():
        z_ref[...] = mul3(ys, ms, NN)

    top = jnp.where(low, base[...], 0.0) - z_ref[:ROWS, :]
    bottom = base[...] - z_ref[ROWS:, :]
    p = onehot_of(ro[...])
    out[...] = pick(jnp.concatenate([top, bottom], axis=0), p, NT)


def level_two(mine, theirs, m, base, a, b, ro):
    return pl.pallas_call(
        level_two_body,
        out_shape=jax.ShapeDtypeStruct((2 * ROWS, F), F32),
        in_specs=[VMEM, VMEM, ANY, VMEM, VMEM, VMEM, VMEM],
        out_specs=VMEM,
        scratch_shapes=[pltpu.VMEM((F, F), F32), pltpu.VMEM((2 * ROWS, F), F32), pltpu.SemaphoreType.DMA((1,))]
        + INVERT_SCRATCH,
        compiler_params=params(56),
        cost_estimate=pl.CostEstimate(flops=40 * 10**9, transcendentals=0, bytes_accessed=12 * 10**6),
        name="level_two",
    )(mine, theirs, m, base, a, b, ro)


def shift(x, by):
    at = lambda z: z % 8 * 2 + z // 8
    return lax.ppermute(x, ("zl", "zh"), [(at((z + by) % 16), at(z)) for z in range(16)])


def shards(row_owner, face_left, face_cross, face_right):
    ro = row_owner.reshape(1, F)
    xl = lax.axis_index("xl")
    send, part = enter(ro, face_left[0, 0], face_cross[0, 0], face_right[0, 0])
    g = lax.all_gather(send, PAIR, axis=1, tiled=True)
    mine = part + lax.ppermute(part, "zh", SWAP)
    ups, downs = [mine], [mine]
    for _ in range(4):
        ups.append(shift(ups[-1], 1))
        if len(downs) < 4:
            downs.append(shift(downs[-1], -1))
    pieces = jnp.concatenate(ups + downs[:0:-1], axis=0)
    si = level_one(pieces, lax.ppermute(pieces, "core", SWAP))
    w, t = products(si, g)
    w2 = lax.ppermute(w, "xl", SWAP)
    m, base, a = between(g, t, si)
    b = lax.ppermute(a, "xl", SWAP)
    w2, m, base, a, b = lax.optimization_barrier((w2, m, base, a, b))
    w = w + w2
    w2 = lax.ppermute(w, "core", SWAP)
    mine = level_two(w, w2, m, base, a, b, ro)
    theirs = lax.ppermute(mine, "xl", SWAP)
    low = xl == 0
    left = jnp.where(low, mine[:ROWS], theirs[:ROWS])
    cross = jnp.where(low, theirs[:ROWS], mine[:ROWS])
    right = jnp.where(low, theirs[ROWS:], mine[ROWS:])
    return (left[None, None], cross[None, None], right[None, None])


def solution(mesh):
    fine = Mesh(mesh.devices.reshape(8, 2, 4, 2, 2, 2), ("zl", "core", "y", "zh", "xh", "xl"))
    face = P(("y", "zh"), ("xh", "xl"), ("zl", "core"), None)
    return jax.shard_map(
        shards, mesh=fine, in_specs=(P(), face, face, face), out_specs=(face, face, face), check_vma=False
    )
```

```python
import functools

import jax
import jax.numpy as jnp
from jax import lax
from jax.experimental import pallas as pl
from jax.experimental.pallas import tpu as pltpu
from jax.sharding import Mesh
from jax.sharding import PartitionSpec as P

F = 768
ROWS = 48
CHUNKED = (16, 2, 24, 768)
B = 128
F32 = jnp.float32
BF16 = jnp.bfloat16
PAIR = ("zh", "zl", "core")
SWAP = [(0, 1), (1, 0)]
VMEM = pl.BlockSpec(memory_space=pltpu.VMEM)
HBM = pl.BlockSpec(memory_space=pltpu.HBM)


def params(mib):
    return pltpu.CompilerParams(vmem_limit_bytes=mib * 1024 * 1024)


def dg(a, b, dims):
    return lax.dot_general(a, b, (dims, ((), ())), preferred_element_type=F32)


NN = ((1,), (0,))
NT = ((1,), (1,))
TN = ((0,), (0,))
TT = ((0,), (1,))


def split3(x):
    h = x.astype(BF16)
    y = x - h.astype(F32)
    m = y.astype(BF16)
    return h, m, (y - m.astype(F32)).astype(BF16)


def mul6(a, b, dims):
    low = (dg(a[2], b[0], dims) + dg(a[0], b[2], dims)) + dg(a[1], b[1], dims)
    return (low + (dg(a[1], b[0], dims) + dg(a[0], b[1], dims))) + dg(a[0], b[0], dims)


def chunks(body):
    def one(j, carry):
        body(pl.ds(pl.multiple_of(j * 256, 256), 256))
        return carry

    lax.fori_loop(0, F // 256, one, 0)


def mul_into(out_ref, x_ref, y_ref, parts):
    for ref, piece in zip(parts, split3(x_ref[...])):
        ref[...] = piece

    def tile(js):
        out_ref[:, js] = mul6([ref[...] for ref in parts], split3(y_ref[:, js]), NN)

    chunks(tile)


def pick(x, onehot, dims):
    h, m, l = split3(x)
    return (dg(l, onehot, dims) + dg(m, onehot, dims)) + dg(h, onehot, dims)


def pick_nt(e, x):
    h, m, l = split3(x)
    return (dg(e, l, NT) + dg(e, m, NT)) + dg(e, h, NT)


def onehot_of(ro):
    c = lax.broadcasted_iota(jnp.int32, (F, F), 0)
    return jnp.where(c == ro, 1.0, 0.0).astype(BF16)


def sub(v, s):
    return jnp.broadcast_to(v[s : s + 1, :], v.shape)


def lane(v, j):
    return jnp.broadcast_to(v[:, j : j + 1], v.shape)


def inv8(b, row):
    b = list(b)
    for p in range(4):
        i, k = 2 * p, 2 * p + 1
        a_, b_, d_ = sub(b[i], i), sub(b[k], i), sub(b[k], k)
        rd = 1.0 / (a_ * d_ - b_ * b_)
        pa, pb, pd = d_ * rd, -b_ * rd, a_ * rd
        ci = jnp.where(row == i, -1.0, jnp.where(row == k, 0.0, b[i]))
        ck = jnp.where(row == k, -1.0, jnp.where(row == i, 0.0, b[k]))
        ui = ci * pa + ck * pb
        uk = ci * pb + ck * pd
        keep = (row != i) & (row != k)
        new = []
        for j in range(8):
            if j == i:
                new.append(-ui)
            elif j == k:
                new.append(-uk)
            else:
                base = jnp.where(keep, b[j], 0.0)
                new.append(base - (ui * sub(b[j], i) + uk * sub(b[j], k)))
        b = new
    return b


def tree(u):
    return ((u[0] + u[1]) + (u[2] + u[3])) + ((u[4] + u[5]) + (u[6] + u[7]))


def inv128(D):
    row = lax.broadcasted_iota(jnp.int32, (8, B), 0)
    col = lax.broadcasted_iota(jnp.int32, (8, B), 1)
    D = list(D)
    for r in range(16):
        rows = D[r]
        ib = inv8([lane(rows, 8 * r + j) for j in range(8)], row)
        inp = (col >= 8 * r) & (col < 8 * r + 8)
        rows = jnp.where(inp, jnp.where(col - 8 * r == row, 1.0, 0.0), rows)
        T = tree([ib[j] * sub(rows, j) for j in range(8)])
        Tj = [sub(T, j) for j in range(8)]
        for q in list(range(r + 1, 16)) + list(range(r)):
            u = tree([lane(D[q], 8 * r + j) * Tj[j] for j in range(8)])
            D[q] = jnp.where(inp, 0.0, D[q]) - u
        D[r] = T
    return D


def cat(*a, axis):
    return jnp.concatenate(a, axis=axis)


def stack6(a):
    a0, a1, a2 = split3(a)
    return cat(a0, a1, axis=1), cat(a0, a2, axis=1)


def mul128(a, b):
    b0, b1, b2 = split3(b)
    low = dg(a[1], cat(b2, b0, axis=0), NN) + dg(a[0], cat(b1, b1, axis=0), NN)
    return low + dg(a[0], cat(b0, b0, axis=0), NN)


def invert(s_ref, d_ref, di_ref, r_ref, c_ref):
    ri = lax.broadcasted_iota(jnp.int32, (B, B), 0)
    ci = lax.broadcasted_iota(jnp.int32, (B, B), 1)
    eye = jnp.where(ri == ci, 1.0, 0.0)
    last = F // B - 1
    di_ref[...] = jnp.zeros((B, B), F32)
    r_ref[...] = jnp.zeros((B, F), F32)
    c_ref[...] = jnp.zeros((F, B), F32)
    d_ref[...] = s_ref[:B, :B]

    def trail(kp):
        T = mul128(stack6(di_ref[...]), r_ref[...])
        c = stack6(c_ref[...])
        for j in range(F // 256):
            js = slice(256 * j, 256 * j + 256)
            s_ref[:F, js] = s_ref[:F, js] - mul128(c, T[:, js])
        s_ref[pl.ds(kp, B), :] = T

    def finish(kp):
        r_ref[...] = mul128(stack6(di_ref[...]), r_ref[...])

        def tile(js):
            s_ref[:F, js] = s_ref[:F, js] - mul128(stack6(c_ref[...]), r_ref[:, js])

        chunks(tile)
        s_ref[pl.ds(kp, B), :] = r_ref[...]

    def step(k, carry):
        ks = pl.multiple_of(k * B, B)
        kp = pl.multiple_of(jnp.where(k == 0, F, ks - B), B)
        kn = pl.multiple_of(jnp.where(k == last, F - B, ks + B), B)
        Di = jnp.concatenate(inv128([d_ref[8 * q : 8 * q + 8, :] for q in range(16)]), axis=0)
        trail(kp)
        rn = s_ref[pl.ds(ks, B), pl.ds(kn, B)]
        cn = s_ref[pl.ds(kn, B), pl.ds(ks, B)]
        dn = s_ref[pl.ds(kn, B), pl.ds(kn, B)]
        c_ref[...] = s_ref[:F, pl.ds(ks, B)]
        c_ref[pl.ds(ks, B), :] = jnp.zeros((B, B), F32)
        r_ref[...] = s_ref[pl.ds(ks, B), :]
        r_ref[:, pl.ds(ks, B)] = eye
        s_ref[:F, pl.ds(ks, B)] = jnp.zeros((F, B), F32)
        di_ref[...] = Di
        d_ref[...] = dn - mul128(stack6(cn), mul128(stack6(Di), rn))
        return carry

    lax.fori_loop(0, last + 1, step, 0)
    finish(F - B)


INVERT_SCRATCH = [
    pltpu.VMEM((F + B, F), F32),
    pltpu.VMEM((B, B), F32),
    pltpu.VMEM((B, B), F32),
    pltpu.VMEM((B, F), F32),
    pltpu.VMEM((F, B), F32),
]


def enter_body(ro, left, cross, right, cross_out, part):
    p = onehot_of(ro[...])
    upper = lax.axis_index("zh") == 1
    l, c, r = left[...], cross[...], right[...]
    part[:ROWS, :] = pick(jnp.where(upper, l, r), p, NN)
    part[ROWS:, :] = pick(jnp.where(upper, r, l), p, NN)
    cross_out[...] = pick(c, p, NN)


def enter(ro, left, cross, right):
    return pl.pallas_call(
        enter_body,
        out_shape=(jax.ShapeDtypeStruct((ROWS, F), F32), jax.ShapeDtypeStruct((2 * ROWS, F), F32)),
        in_specs=[VMEM] * 4,
        out_specs=(VMEM, VMEM),
        compiler_params=params(32),
        name="enter",
    )(ro, left, cross, right)


def level_one_body(mine, theirs, si_out, s_ref, *work):
    core = lax.axis_index("core")
    zl = lax.axis_index("zl")
    for k in range(8):
        at = lax.rem(zl + k, 8) * (2 * ROWS)
        s_ref[pl.ds(pl.multiple_of(at + core * ROWS, ROWS), ROWS), :] = mine[ROWS * k : ROWS * k + ROWS, :]
        s_ref[pl.ds(pl.multiple_of(at + (1 - core) * ROWS, ROWS), ROWS), :] = theirs[ROWS * k : ROWS * k + ROWS, :]
    invert(s_ref, *work)
    si_out[...] = s_ref[:F, :]


def level_one(mine, theirs):
    return pl.pallas_call(
        level_one_body,
        out_shape=jax.ShapeDtypeStruct((F, F), F32),
        in_specs=[VMEM, VMEM],
        out_specs=VMEM,
        scratch_shapes=INVERT_SCRATCH,
        compiler_params=params(56),
        cost_estimate=pl.CostEstimate(flops=40 * 10**9, transcendentals=0, bytes_accessed=5 * 10**6),
        name="level_one",
    )(mine, theirs)


def rows_copy(g, chunk, box, dst, sem):
    return pltpu.make_async_copy(g.at[chunk, box], dst, sem)


def products_body(si, g, w_out, t_out, x4, y4, o4, t_ref, x0, x1, x2, sems):
    low = lax.axis_index("xl") == 0
    first = lax.axis_index("core") == 0
    x_ref, y_ref, o_ref = (r.reshape(F, F) for r in (x4, y4, o4))

    @pl.when(low)
    def _():
        for j in range(2):
            rows_copy(g, j, 1, y4.at[:, j], sems.at[j]).start()
        x_ref[...] = si[...]

    @pl.when(jnp.logical_not(low))
    def _():
        for j in range(2):
            rows_copy(g, j, 0, x4.at[:, j], sems.at[j]).start()
        y_ref[...] = si[...]

    for z in range(2):
        rows_copy(g, 2, z, o4.at[:, z], sems.at[2 + z]).start()
    for j in range(2):
        rows_copy(g, j, 0, x4.at[:, j], sems.at[j]).wait()
    mul_into(t_ref, x_ref, y_ref, (x0, x1, x2))
    out = pltpu.make_async_copy(t_ref, t_out, sems.at[0])
    out.start()
    for z in range(2):
        rows_copy(g, 2, z, o4.at[:, z], sems.at[2 + z]).wait()

    def panels(term):
        def fill(places):
            w_out[...] = jnp.zeros((B, 11 * B), F32)
            for i, at in places:
                w_out[:, at : at + F - B * i] = o_ref[B * i : B * i + B, B * i :]

            def part(ks):
                for i, at in places:
                    here = slice(at, at + F - B * i)
                    w_out[:, here] = w_out[:, here] - term(i, ks)

            chunks(part)

        @pl.when(first)
        def _():
            fill(((0, 0), (1, 768)))

        @pl.when(jnp.logical_not(first))
        def _():
            fill(((2, 0), (3, 512), (4, 896), (5, 1152)))

    @pl.when(low)
    def _():
        panels(lambda i, ks: mul6(split3(y_ref[ks, B * i : B * i + B]), split3(t_ref[ks, B * i :]), TN))

    @pl.when(jnp.logical_not(low))
    def _():
        panels(
            lambda i, ks: mul6(
                split3(t_ref[B * i : B * i + B, ks]), [ref[B * i :, ks] for ref in (x0, x1, x2)], NT
            )
        )

    out.wait()


def products(si, g):
    return pl.pallas_call(
        products_body,
        out_shape=(jax.ShapeDtypeStruct((B, 11 * B), F32), jax.ShapeDtypeStruct((F, F), F32)),
        in_specs=[VMEM, HBM],
        out_specs=(VMEM, HBM),
        scratch_shapes=[pltpu.VMEM(CHUNKED, F32)] * 3
        + [pltpu.VMEM((F, F), F32)]
        + [pltpu.VMEM((F, F), BF16)] * 3
        + [pltpu.SemaphoreType.DMA((4,))],
        compiler_params=params(56),
        cost_estimate=pl.CostEstimate(flops=6 * 10**9, transcendentals=0, bytes_accessed=12 * 10**6),
        name="products",
    )(si, g)


def between_body(g, t, si, keep, m_out, base_out, a_out, x4, y4, m_ref, x0, x1, x2, sems):
    low = lax.axis_index("xl") == 0
    i = (lax.axis_index("zl") * 2 + lax.axis_index("core")) * ROWS
    i = pl.multiple_of(i, ROWS)
    x_ref, y_ref = x4.reshape(F, F), y4.reshape(F, F)

    @pl.when(low)
    def _():
        for j in range(2):
            rows_copy(g, j, 0, x4.at[:, j], sems.at[j]).start()
        pltpu.make_async_copy(t, y4, sems.at[2]).start()

    @pl.when(jnp.logical_not(low))
    def _():
        pltpu.make_async_copy(t, x4, sems.at[2]).start()
        for j in range(2):
            rows_copy(g, j, 1, y4.at[:, j], sems.at[j]).start()

    for j in range(2):
        rows_copy(g, j, 0, x4.at[:, j], sems.at[j]).wait()
    pltpu.make_async_copy(t, x4, sems.at[2]).wait()
    parts = (x0, x1, x2)
    mul_into(m_ref, x_ref, y_ref, parts)
    out = pltpu.make_async_copy(m_ref, m_out, sems.at[0])
    out.start()
    zero = jnp.zeros((ROWS, F), F32)

    def times_inverse(rows):
        a_out[...] = zero

        def part(ks):
            a_out[...] = a_out[...] + mul6(rows(ks), split3(si[ks, :]), NN)

        chunks(part)

    base_out[...] = keep[...]

    @pl.when(low)
    def _():
        times_inverse(lambda ks: [ref[pl.ds(i, ROWS), ks] for ref in parts])

        def part(ks):
            base_out[...] = base_out[...] - mul6(split3(a_out[:, ks]), [ref[:, ks] for ref in parts], NT)

        chunks(part)
        a_out[...] = m_ref[pl.ds(i, ROWS), :]

    @pl.when(jnp.logical_not(low))
    def _():
        r_ = lax.broadcasted_iota(jnp.int32, (ROWS, F), 0) + i
        c_ = lax.broadcasted_iota(jnp.int32, (ROWS, F), 1)
        e = jnp.where(r_ == c_, 1.0, 0.0).astype(BF16)
        times_inverse(lambda ks: [dg(e, p, NT).astype(BF16) for p in split3(y_ref[ks, :])])

        def part(ks):
            base_out[...] = base_out[...] - mul6(split3(a_out[:, ks]), split3(y_ref[ks, :]), NN)

        chunks(part)
        a_out[...] = pick_nt(e, m_ref[...])

    out.wait()


def between(g, t, si, keep):
    rows = jax.ShapeDtypeStruct((ROWS, F), F32)
    return pl.pallas_call(
        between_body,
        out_shape=(jax.ShapeDtypeStruct((F, F), F32), rows, rows),
        in_specs=[HBM, HBM, VMEM, VMEM],
        out_specs=(HBM, VMEM, VMEM),
        scratch_shapes=[pltpu.VMEM(CHUNKED, F32)] * 2
        + [pltpu.VMEM((F, F), F32)]
        + [pltpu.VMEM((F, F), BF16)] * 3
        + [pltpu.SemaphoreType.DMA((3,))],
        compiler_params=params(56),
        cost_estimate=pl.CostEstimate(flops=6 * 10**9, transcendentals=0, bytes_accessed=12 * 10**6),
        name="between",
    )(g, t.reshape(CHUNKED), si, keep)


def level_two_body(mine, theirs, m, base, a, b, ro, out, m_ref, y_ref, z_ref, sems, s_ref, *work):
    gm = pltpu.make_async_copy(m, m_ref, sems.at[0])
    gm.start()
    first = lax.axis_index("core") == 0
    upper = jnp.where(first, mine[...], theirs[...])
    lower = jnp.where(first, theirs[...], mine[...])
    rows = [
        upper[:, :768],
        upper[:, 768:],
        lower[:, :512],
        lower[:, 512:896],
        lower[:, 896:1152],
        lower[:, 1152:1280],
    ]
    for i in range(6):
        s_ref[B * i : B * i + B, B * i :] = rows[i]
        for j in range(i + 1, 6):
            s_ref[B * j : B * j + B, B * i : B * i + B] = rows[i][:, B * (j - i) : B * (j - i) + B].T
    invert(s_ref, *work)
    gm.wait()
    low = lax.axis_index("xl") == 0
    x = jnp.concatenate([jnp.where(low, a[...], b[...]), a[...]], axis=0)
    xs = split3(x)
    y_ref[...] = mul6(xs, split3(s_ref[:F, :]), NN)

    @pl.when(low)
    def _():
        z_ref[...] = mul6(split3(y_ref[...]), split3(m_ref[...]), NT)

    @pl.when(jnp.logical_not(low))
    def _():
        z_ref[...] = mul6(split3(y_ref[...]), split3(m_ref[...]), NN)

    top = jnp.where(low, base[...], 0.0) - z_ref[:ROWS, :]
    bottom = base[...] - z_ref[ROWS:, :]
    p = onehot_of(ro[...])
    out[...] = pick(jnp.concatenate([top, bottom], axis=0), p, NT)


def level_two(mine, theirs, m, base, a, b, ro):
    return pl.pallas_call(
        level_two_body,
        out_shape=jax.ShapeDtypeStruct((2 * ROWS, F), F32),
        in_specs=[VMEM, VMEM, HBM, VMEM, VMEM, VMEM, VMEM],
        out_specs=VMEM,
        scratch_shapes=[pltpu.VMEM((F, F), F32)]
        + [pltpu.VMEM((2 * ROWS, F), F32)] * 2
        + [pltpu.SemaphoreType.DMA((1,))]
        + INVERT_SCRATCH,
        compiler_params=params(56),
        cost_estimate=pl.CostEstimate(flops=40 * 10**9, transcendentals=0, bytes_accessed=12 * 10**6),
        name="level_two",
    )(mine, theirs, m, base, a, b, ro)


def shift(x, by):
    at = lambda z: z % 8 * 2 + z // 8
    return lax.ppermute(x, ("zl", "zh"), [(at((z + by) % 16), at(z)) for z in range(16)])


def shards(row_owner, face_left, face_cross, face_right):
    ro = row_owner.reshape(1, F)
    xl = lax.axis_index("xl")
    zh = lax.axis_index("zh")
    cross, part = enter(ro, face_left[0, 0], face_cross[0, 0], face_right[0, 0])
    partner = lax.ppermute(part, "zh", SWAP)
    mine = part[:ROWS] + partner[:ROWS]
    middle = jnp.where(zh == xl, partner[ROWS:], part[ROWS:])
    keep = jnp.where(zh == xl, part[ROWS:], partner[ROWS:])
    middle = jnp.where(zh == 0, middle[:24], middle[24:])
    g = lax.all_gather(jnp.concatenate([cross, middle]).reshape(3, 24, F), PAIR, axis=1, tiled=True)
    g = g.reshape(3, 2, 16, 24, F)
    ups, downs = [mine], [mine]
    for _ in range(4):
        ups.append(shift(ups[-1], 1))
        if len(downs) < 4:
            downs.append(shift(downs[-1], -1))
    pieces = jnp.concatenate(ups + downs[:0:-1], axis=0)
    si = level_one(pieces, lax.ppermute(pieces, "core", SWAP))
    w, t = products(si, g)
    w2 = lax.ppermute(w, "xl", SWAP)
    m, base, a = between(g, t, si, keep)
    b = lax.ppermute(a, "xl", SWAP)
    w2, m, base, a, b = lax.optimization_barrier((w2, m, base, a, b))
    w = w + w2
    w2 = lax.ppermute(w, "core", SWAP)
    mine = level_two(w, w2, m, base, a, b, ro)
    theirs = lax.ppermute(mine, "xl", SWAP)
    low = xl == 0
    left = jnp.where(low, mine[:ROWS], theirs[:ROWS])
    cross = jnp.where(low, theirs[:ROWS], mine[:ROWS])
    right = jnp.where(low, theirs[ROWS:], mine[ROWS:])
    return (left[None, None], cross[None, None], right[None, None])


def solution(mesh):
    fine = Mesh(mesh.devices.reshape(8, 2, 4, 2, 2, 2), ("zl", "core", "y", "zh", "xh", "xl"))
    face = P(("y", "zh"), ("xh", "xl"), ("zl", "core"), None)
    return jax.shard_map(
        shards, mesh=fine, in_specs=(P(), face, face, face), out_specs=(face, face, face), check_vma=False
    )
```
